128 devices in a mesh: section: 4 (over z), dp: 32 (over y, x, core).
Axes of the slice: x: 4, y: 4, z: 4, core: 2. Of those that a mesh axis runs over, the one named last changes fastest.
Arguments:
- tokens: bfloat16 [256, 32, 3584], P('dp'), may hold values from -6 to 6
- lengths: int32 [256], P('dp'), may hold values from 1 to 32
- assign: int32 [256, 2], P('dp'), may hold values from 0 to 31, as said below
- group_ids: int32 [256], P('dp'), may hold values from 0 to 31
- rewards: float32 [256], P('dp'), may hold values from -6 to 6
- norm_gain: bfloat16 [4, 3584], P('section'), may hold values from 0.5 to 1.5
- w_query: bfloat16 [4, 3584, 1792], P('section', 'dp'), may hold values from -0.09375 to 0.09375
- w_keyval: bfloat16 [4, 3584, 512], P('section', 'dp'), may hold values from -0.09375 to 0.09375
- w_out: bfloat16 [4, 1792, 3584], P('section', 'dp'), may hold values from -0.125 to 0.125
Outputs:
- hidden: bfloat16 [64, 128, 3584], P('dp', None, 'section')
- token_adv: bfloat16 [64, 128], P('dp')
The draws below stay inside these ranges and needn't reach their ends.
Inputs may be any that keep to these rules, and one draw needn't show every extreme that they name: assign[g,0] is one of the 4 dp indices from the sequence's own upward, wrapping; each dp index sends exactly 2 sequences to each of them; assign[g,1] is a row of the owner, and every row of every owner receives exactly 4 sequences.
All inputs are finite; a program needn't handle non-finite values.
Results may differ from the reference program's by a relative error of at most 0.014.
Values may be sent and summed in bfloat16 or wider, within the bound.
A program may use at most 128 MiB of HBM per device.

```python
import math
import jax
import jax.numpy as jnp
from jax import lax

D = 3584
HEADS = 14
KV_HEADS = 2
HEAD = 128
ROW = 128
SEQ_ROW = 4
ROWS_DEV = 2
SEQ_DEV = 8
CAP = 2
LMAX = 32
SEQ_TOT = 256
GROUPS = 32
N_SECTION = 4
N_DP = 32


def draw_assign(key, part):
    sources = SEQ_TOT // SEQ_DEV
    keys_src = jax.random.split(jax.random.fold_in(key, 11), sources)
    send_perm = jax.vmap(lambda one_key: jax.random.permutation(one_key, SEQ_DEV))(keys_src).astype(jnp.int32)
    reach = send_perm // CAP
    source_ids = jnp.arange(sources, dtype=jnp.int32)[:, None]
    owners = (source_ids + reach) % sources
    keys_own = jax.random.split(jax.random.fold_in(key, 12), sources)
    row_perm = jax.vmap(lambda one_key: jax.random.permutation(one_key, SEQ_DEV))(keys_own).astype(jnp.int32)
    target_row = row_perm[owners, send_perm] // SEQ_ROW
    return jnp.stack([owners, target_row], -1).reshape(SEQ_TOT, 2).astype(jnp.int32)


def plant(array, stream_key, least, largest):
    longest = array.shape.index(max(array.shape))
    spots = []
    for shift in (0, 1):
        where = [jax.random.randint(jax.random.fold_in(stream_key, axis), (), 0, length) for axis, length in enumerate(array.shape)]
        where[longest] = (where[longest] + shift) % array.shape[longest]
        spots.append(tuple(where))
    return array.at[spots[0]].set(least).at[spots[1]].set(largest)


def levels(key, extent, shards, least, high):
    def one(dim, parts):
        heights = jax.random.uniform(jax.random.fold_in(jax.random.fold_in(key, 6), dim), (parts,), jnp.float32, least / len(shards), high / len(shards))
        return jnp.repeat(jnp.exp(heights), extent[dim] // parts).reshape((-1,) + (1,) * (len(extent) - dim - 1))

    gain = one(*shards[0])
    for cut in shards[1:]:
        gain = gain * one(*cut)
    return gain


def gaussian(stream_key, extent, deviation, most, cuts=(), kind=jnp.bfloat16):
    drawn = deviation * jax.random.normal(stream_key, extent, jnp.float32)
    if cuts:
        drawn = drawn * levels(stream_key, extent, cuts, -0.22, 0.18)
    return jnp.clip(drawn, -most, most).astype(kind)


def setup_inputs(seed: int = 0) -> dict:
    streams_of = jax.random.split(jax.random.key(seed), 10)
    return {
        "tokens": gaussian(streams_of[0], (SEQ_TOT, LMAX, D), 1.0, 6.0, ((0, 32),)),
        "lengths": plant(jax.random.randint(streams_of[1], (SEQ_TOT,), 1, LMAX + 1), jax.random.fold_in(streams_of[1], 1), 1, LMAX).astype(jnp.int32),
        "assign": draw_assign(jax.random.fold_in(streams_of[9], 71), 0),
        "group_ids": plant(jax.random.randint(streams_of[3], (SEQ_TOT,), 0, GROUPS), jax.random.fold_in(streams_of[3], 1), 0, GROUPS - 1).astype(jnp.int32),
        "rewards": gaussian(streams_of[4], (SEQ_TOT,), 1.0, 6.0, ((0, 32),), jnp.float32),
        "norm_gain": jnp.clip(1.0 + 0.1 * jax.random.normal(streams_of[5], (N_SECTION, D), jnp.float32), 0.5, 1.5).astype(jnp.bfloat16),
        "w_query": gaussian(streams_of[6], (N_SECTION, D, HEADS * HEAD), D ** -0.5, 0.09375, ((0, 4), (1, 32))),
        "w_keyval": gaussian(streams_of[7], (N_SECTION, D, 2 * KV_HEADS * HEAD), D ** -0.5, 0.09375, ((0, 4), (1, 32))),
        "w_out": gaussian(streams_of[8], (N_SECTION, HEADS * HEAD, D), (HEADS * HEAD) ** -0.5, 0.125, ((0, 4), (1, 32))),
    }


EPS = 1e-06
THETA = 1000000.0

def rotate(inputs, position):
    half_size = inputs.shape[-1] // 2
    inverse = THETA ** (-(jnp.arange(half_size, dtype=jnp.float32) * 2.0 / inputs.shape[-1]))
    angles = position.astype(jnp.float32)[..., None] * inverse
    cosine = jnp.cos(angles)[:, :, None, :]
    sine_part = jnp.sin(angles)[:, :, None, :]
    first_half = inputs[..., :half_size]
    second = inputs[..., half_size:]
    return jnp.concatenate([first_half * cosine - second * sine_part, second * cosine + first_half * sine_part], -1)

def attend_block(rows_in, segment, position, gain_row, query_full, keyval_full, out_full):
    count, row_len, width = rows_in.shape
    wide_in = rows_in.astype(jnp.float32)
    variance = lax.optimization_barrier(jnp.mean(wide_in * wide_in, -1, keepdims=True))
    normed = (wide_in * lax.rsqrt(variance + EPS) * gain_row.astype(jnp.float32)).astype(jnp.bfloat16)
    normed = normed.reshape(count * row_len, width)
    head_count = query_full.shape[1] // HEAD
    kv_count = keyval_full.shape[1] // (2 * HEAD)
    per_group = head_count // kv_count
    queries = jnp.dot(normed, query_full, preferred_element_type=jnp.float32).reshape(count, row_len, head_count, HEAD)
    queries = rotate(queries, position).astype(jnp.bfloat16)
    keyval = jnp.dot(normed, keyval_full, preferred_element_type=jnp.float32).reshape(count, row_len, 2, kv_count, HEAD)
    key_rows = rotate(keyval[:, :, 0], position).astype(jnp.bfloat16)
    value_rows = keyval[:, :, 1].astype(jnp.bfloat16)
    grouped = queries.reshape(count, row_len, kv_count, per_group, HEAD)
    scores = jnp.einsum('nqkgd,nskd->nkgqs', grouped.astype(jnp.float32), key_rows.astype(jnp.float32)) / math.sqrt(HEAD)
    columns = jnp.arange(row_len)
    allowed = (segment[:, :, None] == segment[:, None, :]) & (columns[None, None, :] <= columns[None, :, None])
    scores = jnp.where(allowed[:, None, None], scores, -1e+30)
    top_score = lax.optimization_barrier(jnp.max(scores, -1, keepdims=True))
    expo = jnp.exp(scores - top_score)
    weights = (expo / lax.optimization_barrier(jnp.sum(expo, -1, keepdims=True))).astype(jnp.bfloat16)
    mixed_heads = jnp.einsum('nkgqs,nskd->nqkgd', weights.astype(jnp.float32), value_rows.astype(jnp.float32))
    mixed_heads = mixed_heads.astype(jnp.bfloat16).reshape(count * row_len, head_count * HEAD)
    updated = wide_in + jnp.dot(mixed_heads, out_full, preferred_element_type=jnp.float32).reshape(count, row_len, width)
    return updated.astype(jnp.bfloat16)

def reference(tokens, lengths, assign, group_ids, rewards, norm_gain, w_query, w_keyval, w_out):
    total_rows = N_DP * ROWS_DEV
    packed_row = assign[:, 0] * ROWS_DEV + assign[:, 1]
    onehot = (packed_row[:, None] == jnp.arange(total_rows, dtype=jnp.int32)[None, :]).astype(jnp.int32)
    fill = onehot * lengths[:, None]
    running = jnp.cumsum(fill, 0) - fill
    offset = lax.optimization_barrier(jnp.sum(running * onehot, 1)).astype(jnp.int32)
    group_sums = jax.ops.segment_sum(rewards, group_ids, GROUPS)
    counts = jax.ops.segment_sum(jnp.ones_like(rewards), group_ids, GROUPS)
    group_mean = group_sums / jnp.maximum(counts, 1.0)
    adv = (rewards - group_mean[group_ids]).astype(jnp.bfloat16)
    inside_at = jnp.arange(LMAX, dtype=jnp.int32)
    target = packed_row[:, None] * ROW + offset[:, None] + inside_at[None, :]
    target = jnp.where(inside_at[None, :] < lengths[:, None], target, total_rows * ROW).reshape(-1)
    width = tokens.shape[2]
    packed = jnp.zeros((total_rows * ROW, width), jnp.bfloat16).at[target].set(tokens.reshape(-1, width), mode='drop')
    seq_ids = jnp.broadcast_to(jnp.arange(SEQ_TOT, dtype=jnp.int32)[:, None], (SEQ_TOT, LMAX)).reshape(-1)
    segment = jnp.full((total_rows * ROW,), -1, jnp.int32).at[target].set(seq_ids, mode='drop')
    position = jnp.zeros((total_rows * ROW,), jnp.int32).at[target].set(jnp.broadcast_to(inside_at[None, :], (SEQ_TOT, LMAX)).reshape(-1), mode='drop')
    token_adv = jnp.zeros((total_rows * ROW,), jnp.bfloat16).at[target].set(jnp.broadcast_to(adv[:, None], (SEQ_TOT, LMAX)).reshape(-1), mode='drop')
    rows_now = packed.reshape(total_rows, ROW, width)
    segment = segment.reshape(total_rows, ROW)
    position = position.reshape(total_rows, ROW)
    for section_id in range(N_SECTION):
        rows_now = attend_block(rows_now, segment, position, norm_gain[section_id], w_query[section_id], w_keyval[section_id], w_out[section_id])
    return (rows_now, token_adv.reshape(total_rows, ROW))
```

```python
import math

import jax
import jax.numpy as jnp
import numpy as np
from jax import lax
from jax.experimental import pallas as pl
from jax.experimental.pallas import tpu as pltpu
from jax.sharding import PartitionSpec as P

HEAD = 128
ROW = 128
SPREAD = 4
ROWS_DEV = 2
CAP = 2
SECTIONS = 4
WIDTH = 3584
QUARTER = 896
COLS = 1152
QHEADS = 7
EPS = 1e-06
THETA = 1000000.0
MESH = pl.DeviceIdType.MESH
F32 = jnp.float32
BF16 = jnp.bfloat16

CHUNKS = (
    ((0, 0, 56), (0, 56, 56), (1, 0, 56), (1, 56, 56)),
    ((0, 0, 112), (1, 0, 112)),
    ((0, 0, 112), (1, 0, 112)),
    ((0, 0, 112), (1, 0, 112)),
)

ORDER = (
    (("leave", 0), ()),
    (("meta_sibling",), ()),
    (("meta_x",), ()),
    (("tokens",), (
        (("leave_rest", 0),),
        (("leave_rest", 0),),
        (("leave_rest", 0),),
        (("leave_rest", 0),),
    )),
    (("meta_y",), (
        (("root", 0, 0, 0, 56), ("root", 0, 0, 56, 56), ("root", 0, 1, 0, 56), ("root", 0, 1, 56, 56), ("leave", 1), ("leave_rest", 1), ("leave", 2), ("leave_rest", 2), ("leave", 3), ("leave_rest", 3),),
        (("along_y", 0, 0, 0, 56), ("along_y", 0, 0, 56, 56), ("leave", 1), ("leave_rest", 1), ("leave", 2), ("leave_rest", 2), ("leave", 3), ("leave_rest", 3), ("along_y", 0, 1, 0, 56), ("along_y", 0, 1, 56, 56),),
        (("leave", 2), ("leave_rest", 2), ("leave", 3), ("leave_rest", 3),),
        (("along_y", 0, 0, 0, 56), ("along_y", 0, 0, 56, 56), ("leave", 1), ("leave_rest", 1), ("leave", 2), ("leave_rest", 2), ("leave", 3), ("leave_rest", 3), ("along_y", 0, 1, 0, 56), ("along_y", 0, 1, 56, 56),),
    )),
    (("pack",), (
        (("out_x", 0), ("out_x_far", 0), ("root", 1, 0, 0, 112), ("along_x", 0, 0, 0, 56), ("along_x", 0, 0, 56, 56), ("root", 1, 1, 0, 112), ("out_y", 0), ("along_x", 0, 1, 0, 56), ("along_x", 0, 1, 56, 56), ("out_x", 1), ("share", 0, 0, 0, 56), ("share", 0, 0, 56, 56),),
        (("out_x", 0), ("out_x_far", 0), ("along_y", 1, 0, 0, 112), ("along_x", 0, 0, 0, 56), ("along_x", 0, 0, 56, 56), ("along_y", 1, 1, 0, 112), ("out_y", 0), ("along_x", 0, 1, 0, 56), ("along_x", 0, 1, 56, 56), ("out_x", 1), ("share", 0, 0, 0, 56), ("share", 0, 0, 56, 56),),
        (("out_x", 0), ("out_x_far", 0), ("far_y", 0, 0, 0, 56), ("far_y", 0, 0, 56, 56), ("leave", 1), ("leave_rest", 1), ("along_x", 0, 0, 0, 56), ("along_x", 0, 0, 56, 56), ("out_y", 0), ("far_y", 0, 1, 0, 56), ("far_y", 0, 1, 56, 56), ("along_x", 0, 1, 0, 56), ("along_x", 0, 1, 56, 56), ("out_x", 1), ("share", 0, 0, 0, 56), ("share", 0, 0, 56, 56), ("far_y", 1, 0, 0, 112), ("far_y", 1, 1, 0, 112),),
        (("out_x", 0), ("out_x_far", 0), ("along_y", 1, 0, 0, 112), ("along_x", 0, 0, 0, 56), ("along_x", 0, 0, 56, 56), ("along_y", 1, 1, 0, 112), ("out_y", 0), ("along_x", 0, 1, 0, 56), ("along_x", 0, 1, 56, 56), ("out_x", 1), ("share", 0, 0, 0, 56), ("share", 0, 0, 56, 56),),
    )),
    (("pack_tokens",), ()),
    (("partial", 0, 0), ()),
    (("partial", 0, 1), (
        (("root", 2, 0, 0, 112), ("share", 0, 1, 0, 56), ("share", 0, 1, 56, 56), ("out_x_far", 1), ("root", 2, 1, 0, 112),),
        (("last_y", 1, 0, 0, 112), ("share", 0, 1, 0, 56), ("share", 0, 1, 56, 56), ("out_x_far", 1), ("along_y", 2, 0, 0, 112), ("last_y", 1, 1, 0, 112),),
        (("share", 0, 1, 0, 56), ("share", 0, 1, 56, 56), ("out_x_far", 1),),
        (("last_y", 1, 0, 0, 112), ("share", 0, 1, 0, 56), ("share", 0, 1, 56, 56), ("out_x_far", 1), ("along_y", 2, 0, 0, 112), ("last_y", 1, 1, 0, 112),),
    )),
    (("relay", 0), ()),
    (("attend", 0), (
        (("out_y_far", 0), ("along_x", 1, 0, 0, 112), ("out_share", 0), ("out_y", 1), ("out_x", 2), ("along_x", 1, 1, 0, 112),),
        (("out_y_far", 0), ("along_y", 2, 1, 0, 112), ("along_x", 1, 0, 0, 112), ("out_share", 0), ("out_y", 1), ("out_x", 2), ("along_x", 1, 1, 0, 112),),
        (("out_y_far", 0), ("along_x", 1, 0, 0, 112), ("far_y", 2, 0, 0, 112), ("out_share", 0), ("out_y", 1), ("out_x", 2), ("along_x", 1, 1, 0, 112),),
        (("out_y_far", 0), ("along_y", 2, 1, 0, 112), ("along_x", 1, 0, 0, 112), ("out_share", 0), ("out_y", 1), ("out_x", 2), ("along_x", 1, 1, 0, 112),),
    )),
    (("mixed_far", 0), ()),
    (("out_own", 0), (
        (("share", 1, 0, 0, 112), ("root", 3, 0, 0, 112),),
        (("share", 1, 0, 0, 112), ("last_y", 2, 0, 0, 112),),
        (("far_y", 2, 1, 0, 112), ("share", 1, 0, 0, 112),),
        (("share", 1, 0, 0, 112), ("last_y", 2, 0, 0, 112),),
    )),
    (("out_near", 0), (
        (("out_y_far", 1),),
        (("out_y_far", 1),),
        (("out_y_far", 1),),
        (("out_y_far", 1),),
    )),
    (("out_opp", 0), ()),
    (("partial", 1, 0), ()),
    (("partial", 1, 1), (
        (("root", 3, 1, 0, 112), ("share", 1, 1, 0, 112),),
        (("share", 1, 1, 0, 112), ("last_y", 2, 1, 0, 112), ("along_y", 3, 0, 0, 112),),
        (("share", 1, 1, 0, 112),),
        (("share", 1, 1, 0, 112), ("last_y", 2, 1, 0, 112), ("along_y", 3, 0, 0, 112),),
    )),
    (("relay", 1), ()),
    (("attend", 1), (
        (("out_x_far", 2), ("along_x", 2, 0, 0, 112), ("out_share", 1), ("along_x", 2, 1, 0, 112), ("out_y", 2),),
        (("out_x_far", 2), ("along_x", 2, 0, 0, 112), ("out_share", 1), ("along_y", 3, 1, 0, 112), ("along_x", 2, 1, 0, 112), ("out_y", 2),),
        (("out_x_far", 2), ("along_x", 2, 0, 0, 112), ("out_share", 1), ("far_y", 3, 0, 0, 112), ("along_x", 2, 1, 0, 112), ("far_y", 3, 1, 0, 112), ("out_y", 2),),
        (("out_x_far", 2), ("along_x", 2, 0, 0, 112), ("out_share", 1), ("along_y", 3, 1, 0, 112), ("along_x", 2, 1, 0, 112), ("out_y", 2),),
    )),
    (("mixed_far", 1), ()),
    (("out_own", 1), (
        (),
        (("last_y", 3, 0, 0, 112),),
        (),
        (("last_y", 3, 0, 0, 112),),
    )),
    (("out_near", 1), (
        (("share", 2, 0, 0, 112), ("out_x", 3),),
        (("share", 2, 0, 0, 112), ("out_x", 3),),
        (("share", 2, 0, 0, 112), ("out_x", 3),),
        (("share", 2, 0, 0, 112), ("out_x", 3),),
    )),
    (("out_opp", 1), ()),
    (("partial", 2, 0), ()),
    (("partial", 2, 1), (
        (("share", 2, 1, 0, 112), ("out_y_far", 2),),
        (("last_y", 3, 1, 0, 112), ("share", 2, 1, 0, 112), ("out_y_far", 2),),
        (("share", 2, 1, 0, 112), ("out_y_far", 2),),
        (("last_y", 3, 1, 0, 112), ("share", 2, 1, 0, 112), ("out_y_far", 2),),
    )),
    (("relay", 2), ()),
    (("attend", 2), (
        (("along_x", 3, 0, 0, 112), ("out_share", 2), ("along_x", 3, 1, 0, 112), ("out_x_far", 3),),
        (("along_x", 3, 0, 0, 112), ("out_share", 2), ("along_x", 3, 1, 0, 112), ("out_x_far", 3),),
        (("along_x", 3, 0, 0, 112), ("out_share", 2), ("along_x", 3, 1, 0, 112), ("out_x_far", 3),),
        (("along_x", 3, 0, 0, 112), ("out_share", 2), ("along_x", 3, 1, 0, 112), ("out_x_far", 3),),
    )),
    (("mixed_far", 2), ()),
    (("out_own", 2), (
        (("out_y", 3),),
        (("out_y", 3),),
        (("out_y", 3),),
        (("out_y", 3),),
    )),
    (("out_near", 2), (
        (("share", 3, 0, 0, 112),),
        (("share", 3, 0, 0, 112),),
        (("share", 3, 0, 0, 112),),
        (("share", 3, 0, 0, 112),),
    )),
    (("out_opp", 2), ()),
    (("partial", 3, 0), ()),
    (("partial", 3, 1), (
        (("share", 3, 1, 0, 112),),
        (("share", 3, 1, 0, 112),),
        (("share", 3, 1, 0, 112),),
        (("share", 3, 1, 0, 112),),
    )),
    (("relay", 3), ()),
    (("attend", 3), (
        (("out_y_far", 3), ("out_share", 3),),
        (("out_y_far", 3), ("out_share", 3),),
        (("out_y_far", 3), ("out_share", 3),),
        (("out_y_far", 3), ("out_share", 3),),
    )),
    (("mixed_far", 3), ()),
    (("out_own", 3), ()),
    (("out_near", 3), ()),
    (("out_opp", 3), ()),
)

SEQ = 8
LONGEST = 32
N_SLOT = SEQ * LONGEST
TOTAL = 256
N_DP = 32


def mod(a, n):
    return lax.rem(a + 2 * n, n)


class Names:
    def __init__(self):
        self.index = {}

    def __call__(self, *name):
        return self.index.setdefault(name, len(self.index))


def kernel(
    lengths, assign, group_ids, rewards, table, gain_in, wq, wkv, wo, tokens, out, adv_out,
    x, W, WO, G, xg, Pb, R, Fw, ssp, ssr, M, acc, gain, tok, tsend, trecv, meta, bias, cosf, sinf, stage,
    send_sems, recv_sems, local_sems,
):
    z = lax.axis_index("section")
    d = lax.axis_index("dp")
    c = lax.rem(d, 2)
    chip = lax.div(d, 2)
    xx = lax.rem(chip, 4)
    yy = lax.div(chip, 4)
    dy = mod(yy - z, 4)
    is_dy = [dy == k for k in range(4)]
    not_dy = [dy != k for k in range(4)]
    row_me = lax.div(z, 2)
    opp = mod(z + 2, 4)
    up = mod(z + 1, 4)
    down = mod(z - 1, 4)

    def dev(zc, yc, xc, cc):
        return (zc, (yc * 4 + xc) * 2 + cc)

    z_of = lambda zc: (zc, d)
    z_up, z_down = z_of(up), z_of(down)
    x_left, x_right = mod(xx - 1, 4), mod(xx + 1, 4)
    y_low, y_high = mod(yy - 1, 4), mod(yy + 1, 4)
    to_left = dev(z, yy, x_left, c)
    to_right = dev(z, yy, x_right, c)
    to_low = dev(z, y_low, xx, c)
    to_high = dev(z, y_high, xx, c)
    sibling = dev(z, yy, xx, 1 - c)

    rname = Names()
    sname = Names()
    finals = []

    def remote(src, dst, target, rsem, ssem):
        return pltpu.make_async_remote_copy(
            src_ref=src, dst_ref=dst, send_sem=send_sems.at[sname(*ssem)],
            recv_sem=recv_sems.at[rname(*rsem)], device_id=target, device_id_type=MESH,
        )

    def send(make, when=None):
        make().start()
        finals.append((when, make))

    def arrived(ref, *name):
        pltpu.make_async_copy(ref, ref, recv_sems.at[rname(*name)]).wait()

    token_load = pltpu.make_async_copy(
        tokens.at[:, :, pl.ds(pl.multiple_of(z * QUARTER, HEAD), QUARTER)], tok, local_sems.at[0]
    )
    token_load.start()

    barrier = pltpu.get_barrier_semaphore()
    greet = [z_up, z_down, z_of(opp), to_left, to_right, to_low, to_high, sibling]
    greet += [dev(z, yy, mod(xx + 2, 4), c), dev(z, mod(yy + 2, 4), xx, c)]
    greet += [(z, mod(d + t, N_DP)) for t in (1, 2, 3, -1, -2, -3)]
    for target in greet:
        pl.semaphore_signal(barrier, inc=1, device_id=target, device_id_type=MESH)

    def iota(shape, dim):
        return lax.broadcasted_iota(jnp.int32, shape, dim)

    side = QHEADS * HEAD
    for k in range(2):
        stage[k, :, :side] = wq[0, :, k * side : (k + 1) * side]
        for j in range(2):
            at = side + j * HEAD
            head = (2 * j + k) * HEAD
            stage[k, :, at : at + HEAD] = wkv[0, :, head : head + HEAD]
    gain[...] = jnp.broadcast_to(gain_in[...].astype(F32), (8, WIDTH))
    seq, lane = iota((SEQ, HEAD), 0), iota((SEQ, HEAD), 1)
    mine = jnp.zeros((SEQ, HEAD), F32)
    spot = iota((8, N_SLOT), 1)
    seat = jnp.zeros((8, N_SLOT), jnp.int32)
    owners = [assign[0, i] for i in range(SEQ)]
    for i in range(SEQ):
        facts = (
            lengths[i].astype(F32), owners[i].astype(F32), assign[1, i].astype(F32),
            group_ids[i].astype(F32), rewards[i],
        )
        for j, fact in enumerate(facts):
            mine = jnp.where((seq == i) & (lane == j), fact, mine)
        rank = jnp.int32(0)
        for j in range(i):
            rank = rank + (owners[j] == owners[i]).astype(jnp.int32)
        reach = mod(owners[i] - d, N_DP)
        seat = jnp.where(lax.div(spot, LONGEST) == i, (reach * CAP + rank) * LONGEST, seat)
    meta[yy, xx, c] = mine
    goal = (seat + lax.rem(spot, LONGEST))[0:1, :]
    choose = (iota((N_SLOT, N_SLOT), 0) == goal).astype(F32).astype(BF16)
    token_load.wait()
    moved = jnp.dot(
        choose, tok[...].reshape(N_SLOT, QUARTER), preferred_element_type=F32
    ).astype(BF16)
    per = CAP * LONGEST
    trecv[0] = moved[:per]
    for t in range(1, SPREAD):
        tsend[t - 1] = moved[t * per : (t + 1) * per]
    pl.semaphore_wait(barrier, len(greet))

    def meta_sibling():
        def go():
            b = meta.at[yy, xx, c]
            return remote(b, b, sibling, ("MS",), ("MS",))

        send(go)

    def meta_x():
        arrived(meta.at[yy, xx, 1 - c], "MS")
        for t in (1, 3, 2):

            def go(t=t):
                b = meta.at[yy, xx]
                return remote(b, b, dev(z, yy, mod(xx + t, 4), c), ("MX", t), ("MX", t))

            send(go)

    def meta_y():
        for t in (1, 2, 3):
            arrived(meta.at[yy, mod(xx - t, 4)], "MX", t)
        for t in (1, 3, 2):

            def go(t=t):
                b = meta.at[yy]
                return remote(b, b, dev(z, mod(yy + t, 4), xx, c), ("MY", t), ("MY", t))

            send(go)

    def send_tokens():
        for t in range(1, SPREAD):

            def tokens_out(t=t):
                return remote(
                    tsend.at[t - 1], trecv.at[t], (z, mod(d + t, N_DP)), ("T", t), ("T", t)
                )

            send(tokens_out)

    def pack():
        for t in (1, 2, 3):
            arrived(meta.at[mod(yy - t, 4)], "MY", t)
        facts = meta[...].reshape(TOTAL, HEAD)
        turned = facts.T
        length_c, owner_c, row_c, group_c, reward_c = (facts[:, j : j + 1] for j in range(5))
        length_r, owner_r, row_r, group_r, reward_r = (turned[j : j + 1, :] for j in range(5))
        g, h = iota((TOTAL, TOTAL), 0), iota((TOTAL, TOTAL), 1)
        below = h < g

        def total(keep, value):
            return jnp.sum(jnp.where(keep, value, 0.0), 1, keepdims=True)

        same_row = (owner_c * 2.0 + row_c) == (owner_r * 2.0 + row_r)
        offset_c = total(same_row & below, length_r)
        member = group_c == group_r
        adv_c = reward_c - total(member, reward_r) / jnp.maximum(total(member, 1.0), 1.0)
        alike = (owner_c == owner_r) & (lax.div(g, SEQ) == lax.div(h, SEQ)) & below
        rank_c = total(alike, 1.0)
        back = d - lax.div(iota((TOTAL, 1), 0), SEQ)
        back = jnp.where(back < 0, back + N_DP, back).astype(F32)
        slot_c = jnp.where(owner_c == d.astype(F32), back * CAP + rank_c, -1.0)
        slot_of = lax.div(h, LONGEST).astype(F32)
        hit = slot_c == slot_of
        inside = lax.rem(iota((1, TOTAL), 1), LONGEST).astype(F32)
        goal = jnp.sum(jnp.where(hit, row_c * ROW + offset_c, 0.0), 0, keepdims=True) + inside
        room = jnp.sum(jnp.where(hit, length_c, 0.0), 0, keepdims=True)
        goal = jnp.where(inside < room, goal, -1.0)
        place = g.astype(F32) == goal
        spot_c = total(place, h.astype(F32) + 1.0)
        low = jnp.where(row_me == 0, spot_c[:ROW], spot_c[ROW:])
        spot = low.astype(jnp.int32) - 1
        segment_c = jnp.where(spot < 0, -1, lax.div(spot + N_SLOT, LONGEST) - SEQ)
        position_c = jnp.where(spot < 0, 0, lax.rem(spot + N_SLOT, LONGEST))
        column = iota((1, ROW), 1).astype(F32) - offset_c
        within = (column >= 0.0) & (column < length_c) & (slot_c >= 0.0)
        advs = []
        for r in range(ROWS_DEV):
            here = within & (row_c == float(r))
            advs.append(jnp.sum(jnp.where(here, adv_c, 0.0), 0, keepdims=True))
        adv_out[...] = jnp.concatenate(advs, 0).astype(BF16)
        here = within & (row_c == row_me.astype(F32))
        segment_r = jnp.sum(jnp.where(here, slot_c + 1.0, 0.0), 0, keepdims=True) - 1.0
        allowed = (segment_c.astype(F32) == segment_r) & (iota((ROW, ROW), 1) <= iota((ROW, ROW), 0))
        bias[...] = jnp.where(allowed, 0.0, -1e30)
        which = (iota((ROW, LONGEST), 1) == position_c).astype(F32)
        for ref, j in ((cosf, 0), (sinf, 1)):
            ref[...] = jnp.dot(
                which, table[j], precision=lax.Precision.HIGHEST, preferred_element_type=F32
            )
        xg[:, :N_SLOT] = place.astype(F32).astype(BF16)

    def pack_tokens():
        for t in range(1, SPREAD):
            arrived(trecv.at[t], "T", t)
        packed = jnp.dot(
            xg[:, :N_SLOT], trecv[...].reshape(N_SLOT, QUARTER),
            preferred_element_type=F32,
        )
        x[...] = packed.astype(BF16).reshape(ROWS_DEV, ROW, QUARTER)

    def wblock(s, q, xb, cb, lo=0, n=112):
        return W.at[s, q, xb, cb, pl.ds(lo, n)]

    def oblock(s, yb, xb, cb):
        return WO.at[s, lax.div(yb, 2), lax.rem(yb, 2) * 4 + xb, cb]

    def orow(s, yb, cb, lo, n):
        return WO.at[s, lax.div(yb, 2), pl.ds(lax.rem(yb, 2) * 4 + lo, n), cb]

    def halves_of(lo, n):
        first = (n + 8) // 16 * 8
        if lo // 8 % 2:
            first = n - first
        return (lo, first), (lo + first, n - first)

    def leave(s):
        def local(*chunk):
            q, lo, n = chunk
            pltpu.make_async_copy(
                stage.at[mod(q + yy, 2), pl.ds(lo, n)], wblock(s, q, xx, c, lo, n),
                recv_sems.at[rname("Win", s, *chunk)],
            ).start()

        def away(*chunk):
            q, lo, n = chunk
            remote(
                stage.at[mod(q + yy, 2), pl.ds(lo, n)], wblock(s, q, xx, c, lo, n), (yy, d),
                ("Win", s, *chunk), ("Win", s, *chunk),
            ).start()

        def gone(*chunk):
            q, lo, n = chunk
            block = wblock(s, q, xx, c, lo, n)
            pltpu.make_async_copy(block, block, send_sems.at[sname("Win", s, *chunk)]).wait()

        mine = z == s

        @pl.when(mine & (yy == s))
        def _():
            for chunk in CHUNKS[s]:
                local(*chunk)

        @pl.when(mine & (yy != s))
        def _():
            for chunk in CHUNKS[s]:
                away(*chunk)

        def finish():
            @pl.when((z == s) & (yy != s))
            def _():
                for chunk in CHUNKS[s]:
                    gone(*chunk)

        finals.append(finish)

    def leave_rest(s):
        def goto(t):
            dest = (s + t) % 4
            return remote(
                gain.at[:, pl.ds(dest * QUARTER, QUARTER)], G.at[s], (dest, d),
                ("G", s), ("G", s, t),
            )

        def oto(t):
            dest = (s + t) % 4
            return remote(
                wo.at[0, :, pl.ds(dest * QUARTER, QUARTER)], oblock(s, yy, xx, c), (dest, d),
                ("Oin", s), ("Oin", s, t),
            )

        mine = z == s

        @pl.when(mine)
        def _():
            pltpu.make_async_copy(
                gain.at[:, pl.ds(s * QUARTER, QUARTER)], G.at[s], recv_sems.at[rname("G", s)]
            ).start()
            pltpu.make_async_copy(
                wo.at[0, :, pl.ds(s * QUARTER, QUARTER)], oblock(s, yy, xx, c),
                recv_sems.at[rname("Oin", s)],
            ).start()
            for t in (1, 3, 2):
                goto(t).start()
                oto(t).start()

        def finish():
            @pl.when(z == s)
            def _():
                for t in (1, 2, 3):
                    goto(t).wait_send()
                    oto(t).wait_send()

        finals.append(finish)

    def x_sends(s, *chunk):
        q, lo, n = chunk

        def right():
            b = wblock(s, q, xx, c, lo, n)
            return remote(b, b, to_right, ("XL", s, *chunk), ("XL", s, *chunk))

        def left():
            b = wblock(s, q, xx, c, lo, n)
            return remote(b, b, to_left, ("XR", s, *chunk), ("XR", s, *chunk))

        return right, left

    def around_y(s, *chunk):
        q, lo, n = chunk
        near, far = halves_of(lo, n)

        def high():
            b = wblock(s, q, xx, c, *near)
            return remote(b, b, to_high, ("HA", s, *chunk), ("HA", s, *chunk))

        def low():
            b = wblock(s, q, xx, c, *far)
            return remote(b, b, to_low, ("HB", s, *chunk), ("HB", s, *chunk))

        def got_high():
            arrived(wblock(s, q, xx, c, *near), "HA", s, *chunk)

        def got_low():
            arrived(wblock(s, q, xx, c, *far), "HB", s, *chunk)

        return high, low, got_high, got_low

    def root_around(s, *chunk):
        q, lo, n = chunk
        high, low, _, _ = around_y(s, *chunk)
        right, left = x_sends(s, *chunk)

        @pl.when(dy == 0)
        def _():
            arrived(wblock(s, q, xx, c, lo, n), "Win", s, *chunk)
            for f in (high, low, right, left):
                f().start()

        finals.append((not_dy[3], high))
        finals.append((not_dy[1], low))
        finals.append((None, right))
        finals.append((None, left))

    def along_around(s, *chunk):
        high, low, got_high, got_low = around_y(s, *chunk)

        @pl.when(dy == 1)
        def _():
            got_high()
            high().start()

        @pl.when(dy == 3)
        def _():
            got_low()
            low().start()

    def far_around(s, *chunk):
        high, low, got_high, got_low = around_y(s, *chunk)
        right, left = x_sends(s, *chunk)

        @pl.when(dy == 2)
        def _():
            got_high()
            high().start()
            got_low()
            low().start()
            right().start()
            left().start()

    def last_y(s, *chunk):
        _, _, got_high, got_low = around_y(s, *chunk)
        right, left = x_sends(s, *chunk)
        for at, got in ((1, got_low), (3, got_high)):

            @pl.when(dy == at)
            def _():
                got()
                right().start()
                left().start()

    def root(s, *chunk):
        if s > 0:
            return root_around(s, *chunk)
        q, lo, n = chunk

        def high():
            b = wblock(s, q, xx, c, lo, n)
            return remote(b, b, to_high, ("Y", s, *chunk), ("Yh", s, *chunk))

        def low():
            b = wblock(s, q, xx, c, lo, n)
            return remote(b, b, to_low, ("Y", s, *chunk), ("Yl", s, *chunk))

        right, left = x_sends(s, *chunk)

        @pl.when(dy == 0)
        def _():
            arrived(wblock(s, q, xx, c, lo, n), "Win", s, *chunk)
            for f in (high, low, right, left):
                f().start()

        finals.append((is_dy[0], high))
        finals.append((is_dy[0], low))

    def along_y(s, *chunk):
        if s > 0:
            return along_around(s, *chunk)
        q, lo, n = chunk
        near, far = halves_of(lo, n)

        def high():
            b = wblock(s, q, xx, c, *near)
            return remote(b, b, to_high, ("YF0", s, *chunk), ("YF", s, *chunk))

        def low():
            b = wblock(s, q, xx, c, *far)
            return remote(b, b, to_low, ("YF1", s, *chunk), ("YF", s, *chunk))

        right, left = x_sends(s, *chunk)
        for at, forward in ((1, high), (3, low)):

            @pl.when(dy == at)
            def _():
                arrived(wblock(s, q, xx, c, lo, n), "Y", s, *chunk)
                for f in (forward, right, left):
                    f().start()

            finals.append((is_dy[at], forward))

    def far_y(s, *chunk):
        if s > 0:
            return far_around(s, *chunk)
        q, lo, n = chunk
        near, far = halves_of(lo, n)
        right, left = x_sends(s, *chunk)

        @pl.when(dy == 2)
        def _():
            arrived(wblock(s, q, xx, c, *near), "YF0", s, *chunk)
            arrived(wblock(s, q, xx, c, *far), "YF1", s, *chunk)
            right().start()
            left().start()

        finals.append((None, right))
        finals.append((None, left))

    def along_x(s, *chunk):
        q, lo, n = chunk
        near, far = halves_of(lo, n)

        def right():
            b = wblock(s, q, x_left, c, *near)
            return remote(b, b, to_right, ("XF0", s, *chunk), ("XF0", s, *chunk))

        def left():
            b = wblock(s, q, x_right, c, *far)
            return remote(b, b, to_left, ("XF1", s, *chunk), ("XF1", s, *chunk))

        arrived(wblock(s, q, x_left, c, lo, n), "XL", s, *chunk)
        send(right)
        arrived(wblock(s, q, x_right, c, lo, n), "XR", s, *chunk)
        send(left)
        for xb in (xx, x_left, x_right):
            to_sibling(s, q, xb, lo, n).start()

    def to_sibling(s, q, xb, lo, n):
        b = wblock(s, q, xb, c, lo, n)
        return remote(b, b, sibling, ("WD", s, q, lo), ("WD", s, q, lo))

    def share(s, *chunk):
        q, lo, n = chunk
        near, far = halves_of(lo, n)
        b = mod(xx + 2, 4)
        arrived(wblock(s, q, b, c, *near), "XF0", s, *chunk)
        arrived(wblock(s, q, b, c, *far), "XF1", s, *chunk)

        to_sibling(s, q, b, lo, n).start()

        def gone():
            src = W.at[s, q, :, c, pl.ds(lo, n)]
            pltpu.make_async_copy(src, src, send_sems.at[sname("WD", s, q, lo)]).wait()

        finals.append(gone)

    def out_x(s):
        b = oblock(s, yy, xx, c)
        arrived(b, "Oin", s)

        def right():
            b = oblock(s, yy, xx, c)
            return remote(b, b, to_right, ("OXL", s), ("OXL", s))

        def left():
            b = oblock(s, yy, xx, c)
            return remote(b, b, to_left, ("OXR", s), ("OXR", s))

        send(right)
        send(left)

    def out_x_far(s):
        def right():
            b = oblock(s, yy, x_left, c).at[pl.ds(0, 32)]
            return remote(b, b, to_right, ("OXF0", s), ("OXF0", s))

        def left():
            b = oblock(s, yy, x_right, c).at[pl.ds(32, 24)]
            return remote(b, b, to_left, ("OXF1", s), ("OXF1", s))

        arrived(oblock(s, yy, x_left, c), "OXL", s)
        send(right)
        arrived(oblock(s, yy, x_right, c), "OXR", s)
        send(left)

    def out_y(s):
        b = oblock(s, yy, mod(xx + 2, 4), c)
        arrived(b.at[pl.ds(0, 32)], "OXF0", s)
        arrived(b.at[pl.ds(32, 24)], "OXF1", s)

        def high():
            b = orow(s, yy, c, 0, 4)
            return remote(b, b, to_high, ("OYL", s), ("OYL", s))

        def low():
            b = orow(s, yy, c, 0, 4)
            return remote(b, b, to_low, ("OYH", s), ("OYH", s))

        send(high)
        send(low)

    def out_y_far(s):
        def high():
            b = orow(s, y_low, c, 0, 2)
            return remote(b, b, to_high, ("OYF0", s), ("OYF0", s))

        def low():
            b = orow(s, y_high, c, 2, 2)
            return remote(b, b, to_low, ("OYF1", s), ("OYF1", s))

        arrived(orow(s, y_low, c, 0, 4), "OYL", s)
        send(high)
        arrived(orow(s, y_high, c, 0, 4), "OYH", s)
        send(low)

    def out_share(s):
        far = mod(yy + 2, 4)
        arrived(orow(s, far, c, 0, 2), "OYF0", s)
        arrived(orow(s, far, c, 2, 2), "OYF1", s)

        def over():
            src = WO.at[s, :, :, c]
            return remote(src, src, sibling, ("OD", s), ("OD", s))

        send(over)

    def partial(s, q):
        if q == 0:
            arrived(G.at[s], "G", s)
            wide = x[...].reshape(ROWS_DEV * ROW, QUARTER).astype(F32)
            xg[...] = (wide * G[s][0:1, :]).astype(BF16)
        for chunk in CHUNKS[s]:
            if chunk[0] == q:
                _, lo, n = chunk
                arrived(W.at[s, q, :, 1 - c, pl.ds(lo, n)], "WD", s, q, lo)
        k = mod(q + z, 2)
        part = jnp.dot(
            xg[...], W[s, q].reshape(QUARTER, COLS), preferred_element_type=F32
        ).astype(BF16)
        for r in range(ROWS_DEV):
            Pb[s, 2 * r + k] = part[r * ROW : (r + 1) * ROW]
        first = pl.ds(0, 64)
        second = pl.ds(64, 64)
        if q == 0:
            moves = ((opp, first, z_up, 0), (opp, second, z_down, 1))
        else:
            moves = ((up, second, z_up, 2), (down, first, z_down, 3))
        for dest, half, target, slot in moves:

            def move(dest=dest, half=half, target=target, slot=slot):
                return remote(
                    Pb.at[s, dest, half], R.at[s, slot], target, ("R", s, slot), ("R", s, slot)
                )

            send(move)
        if q == 1:
            wide = x[...].reshape(ROWS_DEV * ROW, QUARTER).astype(F32)
            squares = jnp.sum(wide * wide, 1, keepdims=True)
            sums = jnp.broadcast_to(squares, (ROWS_DEV * ROW, HEAD)).T
            for r in range(ROWS_DEV):
                ssp[s, r] = sums[0:8, r * ROW : (r + 1) * ROW]
            for t in (1, 2, 3):
                zt = mod(z + t, 4)

                def ss(t=t, zt=zt):
                    return remote(
                        ssp.at[s, lax.div(zt, 2)], ssr.at[s, t - 1], z_of(zt), ("SS", s, t), ("SS", s, t)
                    )

                send(ss)

    def relay(s):
        for i, (dest, lo, target) in enumerate(((up, 0, z_up), (down, 64, z_down))):
            arrived(R.at[s, i], "R", s, i)
            Fw[s, i] = (
                Pb[s, dest, lo : lo + 64].astype(F32) + R[s, i].astype(F32)
            ).astype(BF16)

            def move(i=i, target=target):
                return remote(Fw.at[s, i], R.at[s, 4 + i], target, ("R", s, 4 + i), ("R", s, 4 + i))

            send(move)

    def attend(s):
        for t in (1, 2, 3):
            arrived(ssr.at[s, t - 1], "SS", s, t)
        total = ssp[s, row_me] + ssr[s, 0] + ssr[s, 1] + ssr[s, 2]
        scale_row = lax.rsqrt(total * (1.0 / WIDTH) + EPS)
        scale = jnp.broadcast_to(scale_row[0:1, :], (ROW, HEAD)).T
        for slot in (2, 3, 4, 5):
            arrived(R.at[s, slot], "R", s, slot)
        own = Pb[s, z].astype(F32)
        upper = own[:64] + R[s, 3].astype(F32) + R[s, 4].astype(F32)
        lower = own[64:] + R[s, 2].astype(F32) + R[s, 5].astype(F32)
        both = jnp.concatenate([upper, lower], 0)
        cosine, sine = cosf[...], sinf[...]
        turned = []
        for h in range(QHEADS + 1):
            t = both[:, h * HEAD : (h + 1) * HEAD] * scale
            turned.append((t * cosine + pltpu.roll(t, 64, 1) * sine).astype(BF16))
        values = (both[:, (QHEADS + 1) * HEAD :] * scale).astype(BF16)
        stacked = jnp.concatenate(turned[:QHEADS], 0)
        scores = lax.dot_general(
            stacked, turned[QHEADS], (((1,), (1,)), ((), ())), preferred_element_type=F32
        ) / math.sqrt(HEAD)
        masked = jnp.concatenate(
            [scores[h * ROW : (h + 1) * ROW] + bias[...] for h in range(QHEADS)], 0
        )
        expo = jnp.exp(masked - jnp.max(masked, -1, keepdims=True))
        weights = (expo / jnp.sum(expo, -1, keepdims=True)).astype(BF16)
        mixed = jnp.dot(weights, values, preferred_element_type=F32).astype(BF16)
        for h in range(QHEADS):
            M[s, z, :, h * HEAD : (h + 1) * HEAD] = mixed[h * ROW : (h + 1) * ROW]
        halves = (pl.ds(0, 64), pl.ds(64, 64))
        for target, side, order in ((z_up, "U", (0, 1)), (z_down, "D", (1, 0))):
            for h in order:

                def move(target=target, side=side, h=h):
                    b = M.at[s, z, halves[h]]
                    return remote(b, b, target, ("M" + side, s, h), ("M" + side, s, h))

                send(move)

    def mixed_far(s):
        arrived(M.at[s, down, pl.ds(0, 64)], "MU", s, 0)

        def on_up():
            b = M.at[s, down, pl.ds(0, 64)]
            return remote(b, b, z_up, ("MF0", s), ("MF0", s))

        send(on_up)
        arrived(M.at[s, up, pl.ds(64, 64)], "MD", s, 1)

        def on_down():
            b = M.at[s, up, pl.ds(64, 64)]
            return remote(b, b, z_down, ("MF1", s), ("MF1", s))

        send(on_down)

    def add_out(s, plane):
        r, k = lax.div(plane, 2), lax.rem(plane, 2)
        acc[r] += jnp.dot(
            M[s, plane], WO[s, k].reshape(QUARTER, QUARTER), preferred_element_type=F32
        )

    def out_own(s):
        arrived(WO.at[s, :, :, 1 - c], "OD", s)
        acc[...] = x[...].astype(F32)
        add_out(s, z)

    def out_near(s):
        arrived(M.at[s, down, pl.ds(64, 64)], "MU", s, 1)
        add_out(s, down)
        arrived(M.at[s, up, pl.ds(0, 64)], "MD", s, 0)
        add_out(s, up)

    def out_opp(s):
        arrived(M.at[s, opp, pl.ds(0, 64)], "MF0", s)
        arrived(M.at[s, opp, pl.ds(64, 64)], "MF1", s)
        add_out(s, opp)
        if s < SECTIONS - 1:
            x[...] = acc[...].astype(BF16)
        else:
            out[...] = acc[...].astype(BF16)

    steps = dict(
        leave=leave, leave_rest=leave_rest, meta_sibling=meta_sibling, meta_x=meta_x, meta_y=meta_y, tokens=send_tokens, pack=pack,
        pack_tokens=pack_tokens, root=root, along_y=along_y, far_y=far_y, last_y=last_y, along_x=along_x,
        share=share, out_x=out_x, out_x_far=out_x_far, out_y=out_y, out_y_far=out_y_far,
        out_share=out_share, partial=partial, relay=relay, attend=attend, out_own=out_own,
        mixed_far=mixed_far, out_near=out_near, out_opp=out_opp,
    )
    seen = set()

    def run(name, *args):
        before = len(finals)
        with jax.named_scope("_".join([name, *map(str, args)])):
            steps[name](*args)
        if (name, *args) in seen:
            del finals[before:]
        seen.add((name, *args))

    for step, gaps in ORDER:
        for k, gap in enumerate(gaps):
            if gap:

                @pl.when(is_dy[k])
                def _():
                    for one in gap:
                        run(*one)

        if step is not None:
            run(*step)
    for item in finals:
        if callable(item):
            item()
            continue
        when, make = item
        if when is None:
            make().wait_send()
        else:

            @pl.when(when)
            def _():
                make().wait_send()


N_SEMS = 340


def hand_over(hidden, token_adv, hidden_out, adv_out):
    hidden_out[...] = hidden[...]
    adv_out[...] = token_adv[...]


def body(tokens, lengths, assign, group_ids, rewards, norm_gain, w_query, w_keyval, w_out):
    inverse = THETA ** (-(np.arange(HEAD // 2) * 2.0 / HEAD))
    angles = np.arange(LONGEST)[:, None] * inverse
    cosine, sine = np.cos(angles), np.sin(angles)
    table = np.stack([np.concatenate([cosine, cosine], 1), np.concatenate([-sine, sine], 1)])
    table = jnp.asarray(table.astype(np.float32))
    vmem = pl.BlockSpec(memory_space=pltpu.VMEM)
    smem = pl.BlockSpec(memory_space=pltpu.SMEM)
    hidden, token_adv = pl.pallas_call(
        kernel,
        out_shape=(
            jax.ShapeDtypeStruct((ROWS_DEV, ROW, QUARTER), BF16),
            jax.ShapeDtypeStruct((ROWS_DEV, ROW), BF16),
        ),
        in_specs=[smem] * 4 + [vmem] * 5 + [pl.BlockSpec(memory_space=pl.ANY)],
        out_specs=(vmem, vmem),
        scratch_shapes=[
            pltpu.VMEM((ROWS_DEV, ROW, QUARTER), BF16),
            pltpu.VMEM((SECTIONS, 2, 4, 2, 112, COLS), BF16),
            pltpu.VMEM((SECTIONS, 2, 8, 2, 56, QUARTER), BF16),
            pltpu.VMEM((SECTIONS, 8, QUARTER), F32),
            pltpu.VMEM((ROWS_DEV * ROW, QUARTER), BF16),
            pltpu.VMEM((SECTIONS, 4, ROW, COLS), BF16),
            pltpu.VMEM((SECTIONS, 6, 64, COLS), BF16),
            pltpu.VMEM((SECTIONS, 2, 64, COLS), BF16),
            pltpu.VMEM((SECTIONS, 2, 8, ROW), F32),
            pltpu.VMEM((SECTIONS, 3, 8, ROW), F32),
            pltpu.VMEM((SECTIONS, 4, ROW, QUARTER), BF16),
            pltpu.VMEM((ROWS_DEV, ROW, QUARTER), F32),
            pltpu.VMEM((8, WIDTH), F32),
            pltpu.VMEM((SEQ, LONGEST, QUARTER), BF16),
            pltpu.VMEM((SPREAD - 1, CAP * LONGEST, QUARTER), BF16),
            pltpu.VMEM((SPREAD, CAP * LONGEST, QUARTER), BF16),
            pltpu.VMEM((4, 4, 2, SEQ, HEAD), F32),
            pltpu.VMEM((ROW, ROW), F32),
            pltpu.VMEM((ROW, HEAD), F32),
            pltpu.VMEM((ROW, HEAD), F32),
            pltpu.VMEM((2, 112, COLS), BF16),
            pltpu.SemaphoreType.DMA((N_SEMS,)),
            pltpu.SemaphoreType.DMA((N_SEMS,)),
            pltpu.SemaphoreType.DMA((1,)),
        ],
        compiler_params=pltpu.CompilerParams(
            collective_id=0, has_side_effects=True, vmem_limit_bytes=64 * 1024 * 1024 - 65536
        ),
    )(lengths, assign.T, group_ids, rewards, table, norm_gain, w_query, w_keyval, w_out, tokens)
    return pl.pallas_call(
        hand_over,
        out_shape=(
            jax.ShapeDtypeStruct(hidden.shape, hidden.dtype),
            jax.ShapeDtypeStruct(token_adv.shape, token_adv.dtype),
        ),
        in_specs=[vmem, vmem],
        out_specs=(vmem, vmem),
    )(hidden, token_adv)


def solution(mesh):
    placed = (
        P("dp", None, None),
        P("dp"),
        P("dp", None),
        P("dp"),
        P("dp"),
        P("section", None),
        P("section", "dp", None),
        P("section", "dp", None),
        P("section", "dp", None),
    )
    return jax.shard_map(
        body,
        mesh=mesh,
        in_specs=placed,
        out_specs=(P("dp", None, "section"), P("dp", None)),
        check_vma=False,
    )
```
